32 devices in a mesh: ap: 16 (over z, x, core), pass: 2 (over y).
Axes of the slice: x: 2, y: 2, z: 4, core: 2. Of those that a mesh axis runs over, the one named last changes fastest.
Arguments:
- echo_record: bfloat16 [2, 16, 2048, 512], P(None, 'pass', 'ap'), may hold values from -6 to 6
- along_track_kernel: bfloat16 [2, 1024, 2048], P(None, None, 'ap'), may hold values from -0.125 to 0.125
- slant_distance_kernel: bfloat16 [2, 512, 256], replicated, may hold values from -0.1875 to 0.1875
- vertical_lags: int32 [16], P('pass'), may hold values from 0 to 128
- lateral_lags: int32 [16], P('pass'), may hold values from 0 to 32
- orbit_source_survey: int32 [16], replicated, may hold values from 0 to 15, each once
- normal_spacings: float32 [16], replicated, may hold values from -1 to 1
Outputs:
- profile: float32 [2, 1024, 256, 512], P(None, ('ap', 'pass'))
The draws below stay inside these ranges and needn't reach their ends.
All inputs are finite; a program needn't handle non-finite values.
Results may differ from the reference program's by a relative error of at most 0.02.
Values may be sent and summed in bfloat16 or wider, within the bound.
A program may use at most 192 MiB of HBM per device.

```python
import jax
import jax.numpy as jnp
from jax import lax

ORBIT_SUM = 16
PULSES = 2048
FREQS = 512
ROWS = 1024
COLS = 256
HEIGHT_CELLS = 512
ITERS = 4
COL_MAX = 32
OFF_MAX = 128


def touch_ends(entries, rng, low, largest):
    index_at = [jax.random.randint(jax.random.fold_in(rng, axis), (), 0, length) for axis, length in enumerate(entries.shape)]
    widest = entries.shape.index(max(entries.shape))
    neighbour = index_at[:widest] + [(index_at[widest] + 1) % entries.shape[widest]] + index_at[widest + 1:]
    return entries.at[tuple(index_at)].set(low).at[tuple(neighbour)].set(largest)


def raised(entries, stream_key, source, target, blocks, factor):
    def block_of(position):
        return (jnp.arange(entries.shape[position]) // (entries.shape[position] // blocks)).reshape((-1,) + (1,) * (entries.ndim - 1 - position))

    near = jax.random.permutation(stream_key, blocks)[block_of(target)]
    other_side = (block_of(target) + blocks // 2) % blocks
    return jnp.where((block_of(source) == near) | (block_of(source) == other_side), factor * entries, entries)


def level_of(rng, dims, cuts, least, largest):
    loudness = 1.0
    for position, parts in cuts:
        draws = jax.random.uniform(jax.random.fold_in(jax.random.fold_in(rng, 6), position), (parts,), jnp.float32, least / len(cuts), largest / len(cuts))
        loudness = loudness * jnp.repeat(jnp.exp(draws), dims[position] // parts).reshape((-1,) + (1,) * (len(dims) - 1 - position))
    return loudness


def normal_values(own_key, extent, width, reach, shards=(), kind=jnp.bfloat16):
    result = jax.random.normal(own_key, extent, jnp.float32) * width
    if len(shards) > 0:
        result = level_of(own_key, extent, shards, -0.22, 0.18) * result
    return jnp.clip(result, min=-reach, max=reach).astype(kind)


def bell_draw_with(key, shape, spread, bound, split, heavy, held_as=jnp.bfloat16):
    array = spread * jax.random.normal(key, shape, jnp.float32)
    if split:
        array = array * level_of(key, shape, split, -0.22, 0.18)
    return jnp.clip(raised(array, jax.random.fold_in(key, 3), *heavy), -bound, bound).astype(held_as)


def setup_inputs(seed: int = 0) -> dict:
    key_of = jax.random.split(jax.random.key(seed), 8)
    return {
        "echo_record": normal_values(key_of[0], (2, ORBIT_SUM, PULSES, FREQS), 1.0, 6.0, ((1, 2), (2, 16))),
        "along_track_kernel": bell_draw_with(key_of[1], (2, ROWS, PULSES), (2 * PULSES) ** -0.5, 0.125, ((2, 16),), (2, 1, 16, 2.0)),
        "slant_distance_kernel": normal_values(key_of[2], (2, FREQS, COLS), (2 * FREQS) ** -0.5, 0.1875),
        "vertical_lags": touch_ends(jax.random.randint(key_of[3], (ORBIT_SUM,), 0, OFF_MAX + 1), jax.random.fold_in(key_of[3], 1), 0, OFF_MAX).astype(jnp.int32),
        "lateral_lags": touch_ends(jax.random.randint(key_of[4], (ORBIT_SUM,), 0, COL_MAX + 1), jax.random.fold_in(key_of[4], 1), 0, COL_MAX).astype(jnp.int32),
        "orbit_source_survey": jax.random.permutation(key_of[5], ORBIT_SUM).astype(jnp.int32),
        "normal_spacings": jnp.clip(jax.random.uniform(key_of[6], (ORBIT_SUM,), jnp.float32, -1.0, 1.0), -1.0, 1.0),
    }


shrink_level = 0.1


def phasor_dictionary(normal_spacings, orbit_source_survey, height_cell_number):
    chosen_height_cells = normal_spacings[orbit_source_survey]
    orbit_start_positions = jnp.arange(height_cell_number).astype(normal_spacings.dtype) - height_cell_number // 2
    phases = jnp.pi * chosen_height_cells[:, None] * orbit_start_positions[None, :]
    return jnp.cos(phases), jnp.sin(phases)


def shrink_steps(obs_re, obs_im, inphase_phasor_part, quadrature_phasor_part):
    passes = inphase_phasor_part.shape[0]
    height_cell_number = inphase_phasor_part.shape[1]
    precise = lax.Precision.HIGHEST
    prof_re = jnp.zeros((obs_re.shape[0], height_cell_number), jnp.float32)
    prof_im = jnp.zeros((obs_re.shape[0], height_cell_number), jnp.float32)
    for sweep_index in range(ITERS):
        if sweep_index == 0:
            resid_re = obs_re
            resid_im = obs_im
        else:
            pred_re = jnp.dot(prof_re, inphase_phasor_part.T, precision=precise) - jnp.dot(prof_im, quadrature_phasor_part.T, precision=precise)
            pred_im = jnp.dot(prof_re, quadrature_phasor_part.T, precision=precise) + jnp.dot(prof_im, inphase_phasor_part.T, precision=precise)
            resid_re = obs_re - pred_re / height_cell_number
            resid_im = obs_im - pred_im / height_cell_number
        grad_re = jnp.dot(resid_re, inphase_phasor_part, precision=precise) + jnp.dot(resid_im, quadrature_phasor_part, precision=precise)
        grad_im = jnp.dot(resid_im, inphase_phasor_part, precision=precise) - jnp.dot(resid_re, quadrature_phasor_part, precision=precise)
        moved_re = prof_re + grad_re / passes
        moved_im = prof_im + grad_im / passes
        prof_re = moved_re - jnp.clip(moved_re, -shrink_level, shrink_level)
        prof_im = moved_im - jnp.clip(moved_im, -shrink_level, shrink_level)
    return prof_re, prof_im


def reference(echo_record, along_track_kernel, slant_distance_kernel, vertical_lags, lateral_lags, orbit_source_survey, normal_spacings):
    def form_pass(inputs):
        planes, row_offset, col_offset = inputs
        focus_re = (jnp.dot(planes[0], slant_distance_kernel[0], preferred_element_type=jnp.float32)
                    - jnp.dot(planes[1], slant_distance_kernel[1], preferred_element_type=jnp.float32)).astype(jnp.bfloat16)
        focus_im = (jnp.dot(planes[0], slant_distance_kernel[1], preferred_element_type=jnp.float32)
                    + jnp.dot(planes[1], slant_distance_kernel[0], preferred_element_type=jnp.float32)).astype(jnp.bfloat16)
        image_re = (jnp.dot(along_track_kernel[0], focus_re, preferred_element_type=jnp.float32)
                    - jnp.dot(along_track_kernel[1], focus_im, preferred_element_type=jnp.float32))
        image_im = (jnp.dot(along_track_kernel[0], focus_im, preferred_element_type=jnp.float32)
                    + jnp.dot(along_track_kernel[1], focus_re, preferred_element_type=jnp.float32))
        stacked = jnp.stack([image_re, image_im])
        padded = jnp.pad(stacked, ((0, 0), (OFF_MAX, 0), (COL_MAX, 0)))
        starts = (jnp.int32(0), (OFF_MAX - row_offset).astype(jnp.int32), (COL_MAX - col_offset).astype(jnp.int32))
        return lax.dynamic_slice(padded, starts, (2, ROWS, COLS)).astype(jnp.bfloat16)

    aligned = lax.map(form_pass, (jnp.moveaxis(echo_record, 1, 0), vertical_lags, lateral_lags))
    inphase_phasor_part, quadrature_phasor_part = phasor_dictionary(normal_spacings, orbit_source_survey, HEIGHT_CELLS)
    blocks = 16
    block_rows = ROWS // blocks
    grouped = jnp.moveaxis(aligned.reshape(ORBIT_SUM, 2, blocks, block_rows * COLS), 2, 0)

    def solve_block(portion):
        values = portion.astype(jnp.float32)
        prof_re, prof_im = shrink_steps(values[:, 0].T, values[:, 1].T, inphase_phasor_part, quadrature_phasor_part)
        return jnp.stack([prof_re, prof_im])

    solved = lax.map(solve_block, grouped)
    return jnp.moveaxis(solved, 1, 0).reshape(2, ROWS, COLS, HEIGHT_CELLS)
```

```python
import functools

import jax
import jax.numpy as jnp
from jax import lax
from jax.experimental import pallas as pl
from jax.experimental.pallas import tpu as pltpu
from jax.sharding import PartitionSpec as P

HEIGHT_CELLS = 512
ITERS = 4
SPAN = 2
CHUNKS = 4
LANES = 256

shrink_level = 0.1


def phasor_dictionary(normal_spacings, orbit_source_survey, height_cell_number):
    support_mask = (
        orbit_source_survey[:, None]
        == jnp.arange(normal_spacings.shape[0], dtype=jnp.int32)[None, :]
    ).astype(normal_spacings.dtype)
    chosen_height_cells = jnp.sum(support_mask * normal_spacings[None, :], axis=1)
    orbit_start_positions = (
        jnp.arange(height_cell_number).astype(normal_spacings.dtype) - height_cell_number // 2
    )
    phases = jnp.pi * chosen_height_cells[:, None] * orbit_start_positions[None, :]
    return (jnp.cos(phases), jnp.sin(phases))


def focus_kernel(lags_ref, echo_ref, slant_ref, out_ref):
    dot = functools.partial(jnp.dot, preferred_element_type=jnp.float32)
    echo_re, echo_im = echo_ref[0, 0], echo_ref[1, 0]
    slant_re, slant_im = slant_ref[0], slant_ref[1]
    lag = lags_ref[pl.program_id(0)]
    focus_re = dot(echo_re, slant_re) - dot(echo_im, slant_im)
    focus_im = dot(echo_re, slant_im) + dot(echo_im, slant_re)
    inside = lax.broadcasted_iota(jnp.int32, focus_re.shape, 1) >= lag
    for plane, values in enumerate((focus_re, focus_im)):
        moved = jnp.where(inside, pltpu.roll(values, lag, 1), 0.0)
        out_ref[plane, 0] = moved.astype(out_ref.dtype)


def focus_range(echo, slant, lateral_lags):
    _, passes, pulses, freqs = echo.shape
    cols = slant.shape[2]
    return pl.pallas_call(
        focus_kernel,
        grid_spec=pltpu.PrefetchScalarGridSpec(
            num_scalar_prefetch=1,
            grid=(passes,),
            in_specs=[
                pl.BlockSpec((2, 1, pulses, freqs), lambda p, lags: (0, p, 0, 0)),
                pl.BlockSpec((2, freqs, cols), lambda p, lags: (0, 0, 0)),
            ],
            out_specs=pl.BlockSpec((2, 1, pulses, cols), lambda p, lags: (0, p, 0, 0)),
        ),
        out_shape=jax.ShapeDtypeStruct((2, passes, pulses, cols), jnp.bfloat16),
        cost_estimate=pl.CostEstimate(
            flops=8 * passes * pulses * freqs * cols,
            bytes_accessed=6 * passes * pulses * freqs,
            transcendentals=0,
        ),
        name="focus",
    )(lateral_lags, echo, slant)


def image_kernel(chunks, pass_count, strip, margin, lags_ref, side_ref, *refs):
    kernels, focuses = refs[0:2], refs[2:4]
    outs, padded = refs[4 : 4 + chunks], refs[4 + chunks]
    owners = outs[0].shape[0]
    rows = kernels[0].shape[1]
    pulses = kernels[0].shape[2]
    cols = outs[0].shape[4]

    @pl.when(pl.program_id(0) == 0)
    def _():
        for s in range(2):
            for plane in range(2):
                padded[2 * s + plane, 0:margin, :] = jnp.zeros((margin, pulses), jnp.float32)
                padded[2 * s + plane, margin : margin + rows, :] = kernels[s][plane].astype(
                    jnp.float32
                )

    base = margin - lags_ref[pl.program_id(0)] + side_ref[0] * strip
    total_re = jnp.zeros((owners * strip, cols), jnp.float32)
    total_im = jnp.zeros((owners * strip, cols), jnp.float32)
    dot = functools.partial(jnp.dot, preferred_element_type=jnp.float32)
    for s in range(2):
        kernel_re, kernel_im = (
            jnp.concatenate(
                [padded[2 * s + plane, pl.ds(base + 2 * o * strip, strip), :] for o in range(owners)],
                axis=0,
            ).astype(jnp.bfloat16)
            for plane in range(2)
        )
        focus_re, focus_im = focuses[s][0, 0], focuses[s][1, 0]
        if pulses % 128 == 0:
            both = jnp.concatenate([kernel_re, kernel_im], axis=1)
            total_re += dot(both, jnp.concatenate([focus_re, -focus_im], axis=0))
            total_im += dot(both, jnp.concatenate([focus_im, focus_re], axis=0))
        else:
            total_re += dot(kernel_re, focus_re) - dot(kernel_im, focus_im)
            total_im += dot(kernel_re, focus_im) + dot(kernel_im, focus_re)
    height = strip // pass_count // chunks
    for plane, total in enumerate((total_re, total_im)):
        if chunks == 1:
            outs[0][:, plane, 0] = total.reshape(owners, strip, cols).astype(jnp.bfloat16)
        else:
            split = total.reshape(owners, pass_count, chunks, height, cols)
            for c in range(chunks):
                outs[c][:, plane, 0] = (
                    split[:, :, c].reshape(owners, pass_count * height, cols).astype(jnp.bfloat16)
                )


def form_images(kernel, kernel_far, focus, focus_far, vertical_lags, side, chunks, pass_count, strip):
    _, rows, pulses = kernel.shape
    passes, cols = focus.shape[1], focus.shape[3]
    owners = rows // strip // 2
    margin = SPAN * strip
    piece = strip // chunks
    whole = pl.BlockSpec((2, rows, pulses), lambda p, *_: (0, 0, 0))
    one = pl.BlockSpec((2, 1, pulses, cols), lambda p, *_: (0, p, 0, 0))
    return pl.pallas_call(
        functools.partial(image_kernel, chunks, pass_count, strip, margin),
        grid_spec=pltpu.PrefetchScalarGridSpec(
            num_scalar_prefetch=2,
            grid=(passes,),
            in_specs=[whole, whole, one, one],
            out_specs=[
                pl.BlockSpec((owners, 2, 1, piece, cols), lambda p, *_: (0, 0, p, 0, 0))
            ]
            * chunks,
            scratch_shapes=[pltpu.VMEM((4, margin + rows, pulses), jnp.float32)],
        ),
        out_shape=[jax.ShapeDtypeStruct((owners, 2, passes, piece, cols), jnp.bfloat16)] * chunks,
        cost_estimate=pl.CostEstimate(
            flops=8 * passes * pulses * rows * cols,
            bytes_accessed=2 * passes * rows * cols,
            transcendentals=0,
        ),
        name="image",
    )(vertical_lags, side, kernel, kernel_far, focus, focus_far)


def shrink_kernel(rows_at_once, y_ref, grad_ref, pred_ref, *refs):
    out_ref = refs[-1]
    cells = out_ref.shape[3]
    cols = out_ref.shape[2]
    width = grad_ref.shape[0]
    block = width // 4
    dot = functools.partial(jnp.dot, preferred_element_type=jnp.float32)
    coarse = (lax.broadcasted_iota(jnp.int32, (cols, width), 1) // block) % 2 == 0
    places = [
        (plane, start) for plane in range(2) for start in range(0, cells, LANES)
    ]
    observed = []
    for i in range(rows_at_once):
        y = y_ref[:, i * cols : (i + 1) * cols].astype(jnp.float32)
        observed.append(jnp.concatenate([y] * 4, axis=0).T)
    resid = list(observed)
    for sweep in range(ITERS):
        for i in range(rows_at_once):
            high = resid[i].astype(jnp.bfloat16)
            low = (resid[i] - high.astype(jnp.float32)).astype(jnp.bfloat16)
            moving = jnp.where(coarse, high, low)
            pred = None
            for n, (plane, start) in enumerate(places):
                v = dot(moving, grad_ref[:, n * LANES : (n + 1) * LANES])
                if sweep > 0:
                    v += out_ref[plane, i, :, start : start + LANES]
                u = v - jnp.clip(v, -shrink_level, shrink_level)
                out_ref[plane, i, :, start : start + LANES] = u
                if sweep < ITERS - 1:
                    part = dot(
                        u.astype(jnp.bfloat16), pred_ref[n * LANES : (n + 1) * LANES, :]
                    )
                    pred = part if pred is None else pred + part
            if sweep < ITERS - 1:
                resid[i] = observed[i] - pred


def shrink_chunk(c, chunks, y, grad, pred, profile, shape):
    _, rows, cols, cells = shape
    height = rows // chunks
    rows_at_once = 2 if height % 2 == 0 else 1
    steps = height // rows_at_once
    width, span = grad.shape
    specs = [
        pl.BlockSpec((y.shape[0], rows_at_once * cols), lambda i: (0, i)),
        pl.BlockSpec((width, span), lambda i: (0, 0)),
        pl.BlockSpec((span, width), lambda i: (0, 0)),
    ]
    operands = [y, grad, pred]
    aliases = {}
    if profile is not None:
        specs.append(pl.BlockSpec(memory_space=pl.ANY))
        operands.append(profile)
        aliases = {3: 0}
    return pl.pallas_call(
        functools.partial(shrink_kernel, rows_at_once),
        grid=(steps,),
        in_specs=specs,
        out_specs=pl.BlockSpec(
            (2, rows_at_once, cols, cells), lambda i: (0, c * steps + i, 0, 0)
        ),
        out_shape=jax.ShapeDtypeStruct(shape, jnp.float32),
        input_output_aliases=aliases,
        cost_estimate=pl.CostEstimate(
            flops=7 * 2 * 8 * height * cols * span * LANES // 8,
            bytes_accessed=8 * height * cols * cells,
            transcendentals=0,
        ),
        name="shrink_%d" % c,
    )(*operands)


def split_high_low(matrix):
    high = matrix.astype(jnp.bfloat16)
    return high, (matrix - high.astype(jnp.float32)).astype(jnp.bfloat16)


def body(
    echo_record,
    along_track_kernel,
    slant_distance_kernel,
    vertical_lags,
    lateral_lags,
    orbit_source_survey,
    normal_spacings,
):
    ap_count = lax.axis_size("ap")
    pass_count = lax.axis_size("pass")
    rows = along_track_kernel.shape[1]
    cols = slant_distance_kernel.shape[2]
    strip = rows // ap_count
    own_rows = strip // pass_count
    chunks = max(1, min(CHUNKS, own_rows // 8))
    passes = normal_spacings.shape[0]
    swap = [(i, i ^ 1) for i in range(ap_count)]
    same_side = [[i for i in range(ap_count) if i % 2 == side] for side in range(2)]

    kernel_far = lax.ppermute(along_track_kernel, "ap", swap)
    focus = focus_range(echo_record, slant_distance_kernel, lateral_lags)
    focus_far = lax.ppermute(focus, "ap", swap)
    side = (lax.axis_index("ap") % 2).astype(jnp.int32).reshape(1)
    pieces = form_images(
        along_track_kernel, kernel_far, focus, focus_far, vertical_lags, side,
        chunks, pass_count, strip,
    )

    inphase, quadrature = phasor_dictionary(normal_spacings, orbit_source_survey, HEIGHT_CELLS)
    adjoint = (
        jnp.concatenate(
            [
                jnp.concatenate([inphase, -quadrature], axis=1),
                jnp.concatenate([quadrature, inphase], axis=1),
            ],
            axis=0,
        )
    )
    grad_high, grad_low = split_high_low(adjoint / passes)
    grad = jnp.concatenate([grad_high, grad_high, grad_low, grad_low], axis=0)
    forward = (adjoint.T / HEIGHT_CELLS).astype(jnp.bfloat16)
    pred = jnp.concatenate([forward] * 4, axis=1)

    profile = None
    shape = (2, own_rows, cols, HEIGHT_CELLS)
    arrived = []
    for piece in pieces:
        arrived.append(
            lax.all_to_all(
                piece, "ap", split_axis=0, concat_axis=0, axis_index_groups=same_side
            )
        )
    for c, received in enumerate(arrived):
        if profile is not None:
            received, profile = lax.optimization_barrier((received, profile))
        summed = jnp.sum(received.astype(jnp.float32), axis=0).astype(jnp.bfloat16)
        stacked = lax.all_to_all(summed, "pass", split_axis=2, concat_axis=1, tiled=True)
        y = stacked.reshape(2 * passes, -1)
        profile = shrink_chunk(c, chunks, y, grad, pred, profile, shape)
    return profile


def solution(mesh):
    return jax.shard_map(
        body,
        mesh=mesh,
        in_specs=(
            P(None, "pass", "ap", None),
            P(None, None, "ap"),
            P(),
            P("pass"),
            P("pass"),
            P(),
            P(),
        ),
        out_specs=P(None, ("ap", "pass"), None, None),
        check_vma=False,
    )
```

```python
import functools

import jax
import jax.numpy as jnp
from jax import lax
from jax.experimental import pallas as pl
from jax.experimental.pallas import tpu as pltpu
from jax.sharding import PartitionSpec as P

HEIGHT_CELLS = 512
ITERS = 4
SPAN = 2
CHUNKS = 4
LANES = 256

shrink_level = 0.1


def phasor_dictionary(normal_spacings, orbit_source_survey, height_cell_number):
    support_mask = (
        orbit_source_survey[:, None]
        == jnp.arange(normal_spacings.shape[0], dtype=jnp.int32)[None, :]
    ).astype(normal_spacings.dtype)
    chosen_height_cells = jnp.sum(support_mask * normal_spacings[None, :], axis=1)
    orbit_start_positions = (
        jnp.arange(height_cell_number).astype(normal_spacings.dtype) - height_cell_number // 2
    )
    phases = jnp.pi * chosen_height_cells[:, None] * orbit_start_positions[None, :]
    return (jnp.cos(phases), jnp.sin(phases))


def focus_kernel(lags_ref, echo_ref, slant_ref, out_ref):
    dot = functools.partial(jnp.dot, preferred_element_type=jnp.float32)
    echo_re, echo_im = echo_ref[0, 0], echo_ref[1, 0]
    slant_re, slant_im = slant_ref[0], slant_ref[1]
    lag = lags_ref[pl.program_id(0)]
    focus_re = dot(echo_re, slant_re) - dot(echo_im, slant_im)
    focus_im = dot(echo_re, slant_im) + dot(echo_im, slant_re)
    inside = lax.broadcasted_iota(jnp.int32, focus_re.shape, 1) >= lag
    for plane, values in enumerate((focus_re, focus_im)):
        moved = jnp.where(inside, pltpu.roll(values, lag, 1), 0.0)
        out_ref[plane, 0] = moved.astype(out_ref.dtype)


def focus_range(echo, slant, lateral_lags):
    _, passes, pulses, freqs = echo.shape
    cols = slant.shape[2]
    return pl.pallas_call(
        focus_kernel,
        grid_spec=pltpu.PrefetchScalarGridSpec(
            num_scalar_prefetch=1,
            grid=(passes,),
            in_specs=[
                pl.BlockSpec((2, 1, pulses, freqs), lambda p, lags: (0, p, 0, 0)),
                pl.BlockSpec((2, freqs, cols), lambda p, lags: (0, 0, 0)),
            ],
            out_specs=pl.BlockSpec((2, 1, pulses, cols), lambda p, lags: (0, p, 0, 0)),
        ),
        out_shape=jax.ShapeDtypeStruct((2, passes, pulses, cols), jnp.bfloat16),
        cost_estimate=pl.CostEstimate(
            flops=8 * passes * pulses * freqs * cols,
            bytes_accessed=6 * passes * pulses * freqs,
            transcendentals=0,
        ),
        name="focus",
    )(lateral_lags, echo, slant)


def image_kernel(direct, chunks, pass_count, strip, margin, lags_ref, side_ref, *refs):
    kernels, focuses = refs[0:2], refs[2:4]
    outs, padded = refs[4:-1], refs[-1]
    owners = kernels[0].shape[1] // strip // 2
    rows = kernels[0].shape[1]
    pulses = kernels[0].shape[2]
    cols = outs[0].shape[-1]

    @pl.when(pl.program_id(0) == 0)
    def _():
        for s in range(2):
            for plane in range(2):
                padded[2 * s + plane, 0:margin, :] = jnp.zeros((margin, pulses), jnp.float32)
                padded[2 * s + plane, margin : margin + rows, :] = kernels[s][plane].astype(
                    jnp.float32
                )

    base = margin - lags_ref[pl.program_id(0)] + side_ref[0] * strip
    half = strip // pass_count
    starts = []
    for o in range(owners):
        if direct:
            first = base + 2 * lax.rem(side_ref[1] + o, owners) * strip
            for q in range(pass_count):
                starts.append((first + lax.rem(side_ref[2] + q, pass_count) * half, half))
        else:
            starts.append((base + 2 * o * strip, strip))
    total_re = jnp.zeros((owners * strip, cols), jnp.float32)
    total_im = jnp.zeros((owners * strip, cols), jnp.float32)
    dot = functools.partial(jnp.dot, preferred_element_type=jnp.float32)
    for s in range(2):
        kernel_re, kernel_im = (
            jnp.concatenate(
                [padded[2 * s + plane, pl.ds(start, size), :] for start, size in starts],
                axis=0,
            ).astype(jnp.bfloat16)
            for plane in range(2)
        )
        focus_re, focus_im = focuses[s][0, 0], focuses[s][1, 0]
        if pulses % 128 == 0:
            both = jnp.concatenate([kernel_re, kernel_im], axis=1)
            total_re += dot(both, jnp.concatenate([focus_re, -focus_im], axis=0))
            total_im += dot(both, jnp.concatenate([focus_im, focus_re], axis=0))
        else:
            total_re += dot(kernel_re, focus_re) - dot(kernel_im, focus_im)
            total_im += dot(kernel_re, focus_im) + dot(kernel_im, focus_re)
    height = strip // pass_count // chunks
    for plane, total in enumerate((total_re, total_im)):
        if chunks == 1 and not direct:
            outs[0][:, plane, 0] = total.reshape(owners, strip, cols).astype(jnp.bfloat16)
        else:
            split = total.reshape(owners, pass_count, chunks, height, cols)
            for c in range(chunks):
                part = split[:, :, c].reshape(owners, pass_count * height, cols)
                part = part.astype(jnp.bfloat16)
                if direct:
                    for o in range(owners):
                        outs[c * owners + o][plane, 0] = part[o]
                else:
                    outs[c][:, plane, 0] = part


def form_images(direct, kernel, kernel_far, focus, focus_far, vertical_lags, side, chunks, pass_count, strip):
    _, rows, pulses = kernel.shape
    passes, cols = focus.shape[1], focus.shape[3]
    owners = rows // strip // 2
    margin = SPAN * strip
    piece = strip // chunks
    whole = pl.BlockSpec((2, rows, pulses), lambda p, *_: (0, 0, 0))
    one = pl.BlockSpec((2, 1, pulses, cols), lambda p, *_: (0, p, 0, 0))
    if direct:
        out_specs = [pl.BlockSpec((2, 1, piece, cols), lambda p, *_: (0, p, 0, 0))]
        out_shape = [jax.ShapeDtypeStruct((2, passes, piece, cols), jnp.bfloat16)]
        out_specs, out_shape = out_specs * (chunks * owners), out_shape * (chunks * owners)
    else:
        out_specs = [pl.BlockSpec((owners, 2, 1, piece, cols), lambda p, *_: (0, 0, p, 0, 0))]
        out_shape = [jax.ShapeDtypeStruct((owners, 2, passes, piece, cols), jnp.bfloat16)]
        out_specs, out_shape = out_specs * chunks, out_shape * chunks
    return pl.pallas_call(
        functools.partial(image_kernel, direct, chunks, pass_count, strip, margin),
        grid_spec=pltpu.PrefetchScalarGridSpec(
            num_scalar_prefetch=2,
            grid=(passes,),
            in_specs=[whole, whole, one, one],
            out_specs=out_specs,
            scratch_shapes=[pltpu.VMEM((4, margin + rows, pulses), jnp.float32)],
        ),
        out_shape=out_shape,
        cost_estimate=pl.CostEstimate(
            flops=8 * passes * pulses * rows * cols,
            bytes_accessed=2 * passes * rows * cols,
            transcendentals=0,
        ),
        name="image",
    )(vertical_lags, side, kernel, kernel_far, focus, focus_far)


def shrink_kernel(rows_at_once, y_ref, grad_ref, pred_ref, *refs):
    out_ref = refs[-1]
    cells = out_ref.shape[3]
    cols = out_ref.shape[2]
    width = grad_ref.shape[0]
    block = width // 4
    dot = functools.partial(jnp.dot, preferred_element_type=jnp.float32)
    coarse = (lax.broadcasted_iota(jnp.int32, (cols, width), 1) // block) % 2 == 0
    places = [
        (plane, start) for plane in range(2) for start in range(0, cells, LANES)
    ]
    observed = []
    for i in range(rows_at_once):
        y = y_ref[:, i * cols : (i + 1) * cols].astype(jnp.float32)
        observed.append(jnp.concatenate([y] * 4, axis=0).T)
    resid = list(observed)
    for sweep in range(ITERS):
        for i in range(rows_at_once):
            high = resid[i].astype(jnp.bfloat16)
            low = (resid[i] - high.astype(jnp.float32)).astype(jnp.bfloat16)
            moving = jnp.where(coarse, high, low)
            pred = None
            for n, (plane, start) in enumerate(places):
                v = dot(moving, grad_ref[:, n * LANES : (n + 1) * LANES])
                if sweep > 0:
                    v += out_ref[plane, i, :, start : start + LANES]
                u = v - jnp.clip(v, -shrink_level, shrink_level)
                out_ref[plane, i, :, start : start + LANES] = u
                if sweep < ITERS - 1:
                    part = dot(
                        u.astype(jnp.bfloat16), pred_ref[n * LANES : (n + 1) * LANES, :]
                    )
                    pred = part if pred is None else pred + part
            if sweep < ITERS - 1:
                resid[i] = observed[i] - pred


def shrink_chunk(c, chunks, y, grad, pred, profile, shape):
    _, rows, cols, cells = shape
    height = rows // chunks
    rows_at_once = 2 if height % 2 == 0 else 1
    steps = height // rows_at_once
    width, span = grad.shape
    specs = [
        pl.BlockSpec((y.shape[0], rows_at_once * cols), lambda i: (0, i)),
        pl.BlockSpec((width, span), lambda i: (0, 0)),
        pl.BlockSpec((span, width), lambda i: (0, 0)),
    ]
    operands = [y, grad, pred]
    aliases = {}
    if profile is not None:
        specs.append(pl.BlockSpec(memory_space=pl.ANY))
        operands.append(profile)
        aliases = {3: 0}
    return pl.pallas_call(
        functools.partial(shrink_kernel, rows_at_once),
        grid=(steps,),
        in_specs=specs,
        out_specs=pl.BlockSpec(
            (2, rows_at_once, cols, cells), lambda i: (0, c * steps + i, 0, 0)
        ),
        out_shape=jax.ShapeDtypeStruct(shape, jnp.float32),
        input_output_aliases=aliases,
        cost_estimate=pl.CostEstimate(
            flops=7 * 2 * 8 * height * cols * span * LANES // 8,
            bytes_accessed=8 * height * cols * cells,
            transcendentals=0,
        ),
        name="shrink_%d" % c,
    )(*operands)


def split_high_low(matrix):
    high = matrix.astype(jnp.bfloat16)
    return high, (matrix - high.astype(jnp.float32)).astype(jnp.bfloat16)


def body(
    echo_record,
    along_track_kernel,
    slant_distance_kernel,
    vertical_lags,
    lateral_lags,
    orbit_source_survey,
    normal_spacings,
):
    ap_count = lax.axis_size("ap")
    pass_count = lax.axis_size("pass")
    rows = along_track_kernel.shape[1]
    cols = slant_distance_kernel.shape[2]
    strip = rows // ap_count
    own_rows = strip // pass_count
    chunks = max(1, min(CHUNKS, own_rows // 8))
    passes = normal_spacings.shape[0]
    swap = [(i, i ^ 1) for i in range(ap_count)]
    same_side = [[i for i in range(ap_count) if i % 2 == side] for side in range(2)]

    kernel_far = lax.ppermute(along_track_kernel, "ap", swap)
    focus = focus_range(echo_record, slant_distance_kernel, lateral_lags)
    focus_far = lax.ppermute(focus, "ap", swap)
    place, own_pass = lax.axis_index("ap"), lax.axis_index("pass")
    side = jnp.stack([place % 2, place // 2, own_pass]).astype(jnp.int32)
    direct = pass_count == 2 and own_rows % 8 == 0
    if direct:
        orbit_source_survey = jnp.where(
            own_pass == 0, orbit_source_survey, jnp.roll(orbit_source_survey, passes // 2)
        )
    pieces = form_images(
        direct, along_track_kernel, kernel_far, focus, focus_far, vertical_lags, side,
        chunks, pass_count, strip,
    )

    inphase, quadrature = phasor_dictionary(normal_spacings, orbit_source_survey, HEIGHT_CELLS)
    adjoint = (
        jnp.concatenate(
            [
                jnp.concatenate([inphase, -quadrature], axis=1),
                jnp.concatenate([quadrature, inphase], axis=1),
            ],
            axis=0,
        )
    )
    grad_high, grad_low = split_high_low(adjoint / passes)
    grad = jnp.concatenate([grad_high, grad_high, grad_low, grad_low], axis=0)
    forward = (adjoint.T / HEIGHT_CELLS).astype(jnp.bfloat16)
    pred = jnp.concatenate([forward] * 4, axis=1)

    profile = None
    shape = (2, own_rows, cols, HEIGHT_CELLS)
    if direct:
        owners = ap_count // 2
        height = strip // chunks // 2
        arrived = []
        for c in range(chunks):
            received = [pieces[c * owners]]
            for d in range(1, owners):
                ring = [(i, (i + 2 * d) % ap_count) for i in range(ap_count)]
                received.append(lax.ppermute(pieces[c * owners + d], "ap", ring))
            arrived.append(received)
        for c, received in enumerate(arrived):
            if c > 0:
                received, profile = lax.optimization_barrier((received, profile))
            summed = sum(r.astype(jnp.float32) for r in received).astype(jnp.bfloat16)
            theirs = lax.ppermute(summed[:, :, height:], "pass", [(0, 1), (1, 0)])
            stacked = jnp.concatenate([summed[:, :, :height], theirs], axis=1)
            y = stacked.reshape(2 * passes, -1)
            if profile is not None:
                y, profile = lax.optimization_barrier((y, profile))
            profile = shrink_chunk(c, chunks, y, grad, pred, profile, shape)
        return profile
    arrived = []
    for piece in pieces:
        arrived.append(
            lax.all_to_all(
                piece, "ap", split_axis=0, concat_axis=0, axis_index_groups=same_side
            )
        )
    for c, received in enumerate(arrived):
        if profile is not None:
            received, profile = lax.optimization_barrier((received, profile))
        summed = jnp.sum(received.astype(jnp.float32), axis=0).astype(jnp.bfloat16)
        stacked = lax.all_to_all(summed, "pass", split_axis=2, concat_axis=1, tiled=True)
        y = stacked.reshape(2 * passes, -1)
        profile = shrink_chunk(c, chunks, y, grad, pred, profile, shape)
    return profile


def solution(mesh):
    return jax.shard_map(
        body,
        mesh=mesh,
        in_specs=(
            P(None, "pass", "ap", None),
            P(None, None, "ap"),
            P(),
            P("pass"),
            P("pass"),
            P(),
            P(),
        ),
        out_specs=P(None, ("ap", "pass"), None, None),
        check_vma=False,
    )
```
